32 devices in a mesh: dp: 4 (over y, z), tp: 8 (over x, core).
Axes of the slice: x: 4, y: 2, z: 2, core: 2. Of those that a mesh axis runs over, the one named last changes fastest.
The devices are a block of a 4x4x8 slice.
Arguments:
- hidden: bfloat16 [16384, 1536], P(('dp', 'tp')), parts along dimension 0
- routes: int32 [2, 16384], P(None, ('dp', 'tp')), parts along dimension 1
- w_query: bfloat16 [2, 1536, 1536], P(None, None, 'tp')
- w_key: bfloat16 [1536, 512], P(None, 'tp')
- w_value: bfloat16 [1536, 512], P(None, 'tp')
- w_out: bfloat16 [2, 1536, 1536], P(None, 'tp')
- q_gain: float32 [2, 64], replicated
- k_gain: float32 [64], replicated
- w_router: bfloat16 [2, 1536, 40], replicated
- shared_gate: bfloat16 [2, 1536, 512], P(None, None, 'tp')
- shared_up: bfloat16 [2, 1536, 512], P(None, None, 'tp')
- shared_down: bfloat16 [2, 512, 1536], P(None, 'tp')
- expert_gate: bfloat16 [2, 40, 1536, 512], P(None, None, None, 'tp')
- expert_up: bfloat16 [2, 40, 1536, 512], P(None, None, None, 'tp')
- expert_down: bfloat16 [2, 40, 512, 1536], P(None, None, 'tp')
Outputs:
- output 1: bfloat16 [16384, 1536], P(('dp', 'tp')), parts along dimension 0
- output 2: bfloat16 [16384, 8, 64], P('dp', 'tp'), parts along dimension 0
- output 3: bfloat16 [16384, 8, 64], P('dp', 'tp'), parts along dimension 0
There are 4 independent parts. The reference program is written for one: setup_inputs(seed, part) draws one part's arguments, and reference() takes and returns one part's arrays. A program takes and returns all parts, laid end to end along the dimension named above; an argument that names none is the same for every part.
All inputs are finite; a program needn't handle non-finite values.
Results may differ from the reference program's by a relative error of at most 0.02.
Values are sent between devices in bfloat16 or wider.
A program may use at most 768 MiB of HBM per device.

```python
import jax
import jax.numpy as jnp
from jax import lax

D = 1536
HEADS = 24
KV_HEADS = 8
HEAD = 64
EXPERTS = 40
FF = 512
SEQ = 4096
Q_BLOCK = 256
ROW_BLOCK = 128

EPS = 1e-5
ROPE_BASE = 10000.0


def draw_routes(key):
    keys = jax.random.split(key, 4)
    skewed = jax.random.randint(keys[0], (2, SEQ), 0, EXPERTS)
    skewed = jnp.minimum(skewed, jax.random.randint(keys[1], (2, SEQ), 0, EXPERTS))
    skewed = jnp.minimum(skewed, jax.random.randint(keys[2], (2, SEQ), 0, EXPERTS))
    forced_pos = jnp.stack([jax.random.permutation(jax.random.fold_in(keys[3], layer), SEQ)[:EXPERTS] for layer in range(2)])
    layer_rows = jnp.arange(2)[:, None]
    expert_ids = jnp.broadcast_to(jnp.arange(EXPERTS, dtype=jnp.int32)[None, :], (2, EXPERTS))
    return skewed.at[layer_rows, forced_pos].set(expert_ids)


def setup_inputs(seed: int = 0, part: int = 0) -> dict:
    base_key = jax.random.key(seed)
    part_key = jax.random.fold_in(base_key, part)
    weight_keys = jax.random.split(jax.random.fold_in(base_key, 1000), 16)

    def normal(key_index, arr_shape, scale):
        return (jax.random.normal(weight_keys[key_index], arr_shape, jnp.float32) * scale).astype(jnp.bfloat16)

    q_width = HEADS * HEAD
    kv_width = KV_HEADS * HEAD
    hidden = jax.random.normal(jax.random.fold_in(part_key, 1), (SEQ, D), jnp.float32).astype(jnp.bfloat16)
    return {
        "hidden": hidden,
        "routes": draw_routes(jax.random.fold_in(part_key, 2)),
        "w_query": normal(0, (2, D, q_width), D ** -0.5),
        "w_key": normal(1, (D, kv_width), D ** -0.5),
        "w_value": normal(2, (D, kv_width), D ** -0.5),
        "w_out": normal(3, (2, q_width, D), 2.0 * q_width ** -0.5),
        "q_gain": jax.random.uniform(weight_keys[4], (2, HEAD), jnp.float32, 1.0, 2.0),
        "k_gain": jax.random.uniform(weight_keys[5], (HEAD,), jnp.float32, 1.0, 2.0),
        "w_router": normal(6, (2, D, EXPERTS), D ** -0.5),
        "shared_gate": normal(7, (2, D, FF), D ** -0.5),
        "shared_up": normal(8, (2, D, FF), D ** -0.5),
        "shared_down": normal(9, (2, FF, D), FF ** -0.5),
        "expert_gate": normal(10, (2, EXPERTS, D, FF), D ** -0.5),
        "expert_up": normal(11, (2, EXPERTS, D, FF), D ** -0.5),
        "expert_down": normal(12, (2, EXPERTS, FF, D), (EXPERTS / FF) ** 0.5),
    }


def rms_norm(vals):
    vals = vals.astype(jnp.float32)
    return vals * lax.rsqrt(jnp.mean(vals * vals, axis=-1, keepdims=True) + EPS)


def rope_tables():
    half_dim = HEAD // 2
    inv_freq = ROPE_BASE ** (-2.0 * jnp.arange(half_dim, dtype=jnp.float32) / HEAD)
    angles = jnp.arange(SEQ, dtype=jnp.float32)[:, None] * inv_freq[None, :]
    return jnp.cos(angles)[:, None, :], jnp.sin(angles)[:, None, :]


def rope_norm(vals, cos_t, sin_t, gain):
    vals = vals.astype(jnp.float32)
    half_dim = HEAD // 2
    first, second = vals[..., :half_dim], vals[..., half_dim:]
    rotated = jnp.concatenate([first * cos_t - second * sin_t, second * cos_t + first * sin_t], axis=-1)
    return (rms_norm(rotated) * gain).astype(jnp.bfloat16)


def attention(q_n, k_n, v_heads):
    q_per_kv = HEADS // KV_HEADS
    n_blocks = SEQ // Q_BLOCK
    q_blocks = q_n.astype(jnp.float32).reshape(n_blocks, Q_BLOCK, KV_HEADS, q_per_kv, HEAD)
    keys_f = k_n.astype(jnp.float32)
    values_f = v_heads.astype(jnp.float32)
    key_pos = jnp.arange(SEQ)

    def one_block(operands):
        q_blk, blk_start = operands
        scores = jnp.einsum("qkgd,skd->kgqs", q_blk, keys_f) * HEAD ** -0.5
        causal_mask = key_pos[None, :] <= (blk_start + jnp.arange(Q_BLOCK))[:, None]
        attn_probs = jax.nn.softmax(jnp.where(causal_mask, scores, -jnp.inf), axis=-1)
        attn_probs = attn_probs.astype(jnp.bfloat16).astype(jnp.float32)
        blk_out = jnp.einsum("kgqs,skd->qkgd", attn_probs, values_f)
        return blk_out.reshape(Q_BLOCK, HEADS * HEAD).astype(jnp.bfloat16)

    blk_outs = lax.map(one_block, (q_blocks, jnp.arange(n_blocks) * Q_BLOCK))
    return blk_outs.reshape(SEQ, HEADS * HEAD)


def routed_experts(n_act, route, e_gate, e_up, e_down):
    counts = jnp.zeros((EXPERTS,), jnp.int32).at[route].add(1)
    order = jnp.argsort(route, stable=True)
    sorted_ids = route[order]
    starts = jnp.cumsum(counts) - counts
    blocks_each = (counts + ROW_BLOCK - 1) // ROW_BLOCK
    block_start = jnp.cumsum(blocks_each) - blocks_each
    dest_row = block_start[sorted_ids] * ROW_BLOCK + jnp.arange(SEQ) - starts[sorted_ids]
    n_blocks = SEQ // ROW_BLOCK + EXPERTS
    padded = jnp.zeros((n_blocks * ROW_BLOCK, D), jnp.bfloat16).at[dest_row].set(n_act[order])
    block_ids = jnp.arange(n_blocks)
    block_expert = jnp.minimum(jnp.sum((block_start[None, :] <= block_ids[:, None]).astype(jnp.int32), axis=1) - 1, EXPERTS - 1)

    def one_block(operands):
        blk_rows, expert = operands
        gate_part = jnp.dot(blk_rows, e_gate[expert], preferred_element_type=jnp.float32)
        up_part = jnp.dot(blk_rows, e_up[expert], preferred_element_type=jnp.float32)
        mid_act = (jax.nn.silu(gate_part) * up_part).astype(jnp.bfloat16)
        return jnp.dot(mid_act, e_down[expert], preferred_element_type=jnp.float32)

    block_out = lax.map(one_block, (padded.reshape(n_blocks, ROW_BLOCK, D), block_expert))
    sorted_out = block_out.reshape(n_blocks * ROW_BLOCK, D)[dest_row]
    return jnp.zeros((SEQ, D), jnp.float32).at[order].set(sorted_out)


def moe_block(state, route, router_w, s_gate, s_up, s_down, e_gate, e_up, e_down):
    n_act = rms_norm(state).astype(jnp.bfloat16)
    router_probs = jax.nn.softmax(jnp.dot(n_act, router_w, preferred_element_type=jnp.float32), axis=-1)
    gate_val = jnp.sum(jnp.where(route[:, None] == jnp.arange(EXPERTS)[None, :], router_probs, 0.0), axis=1)
    shared_mid = (jax.nn.silu(jnp.dot(n_act, s_gate, preferred_element_type=jnp.float32)) * jnp.dot(n_act, s_up, preferred_element_type=jnp.float32)).astype(jnp.bfloat16)
    shared_out = jnp.dot(shared_mid, s_down, preferred_element_type=jnp.float32)
    routed_out = routed_experts(n_act, route, e_gate, e_up, e_down)
    return (state.astype(jnp.float32) + shared_out + gate_val[:, None] * routed_out).astype(jnp.bfloat16)


def reference(hidden, routes, w_query, w_key, w_value, w_out, q_gain, k_gain, w_router, shared_gate, shared_up, shared_down, expert_gate, expert_up, expert_down):
    cos_t, sin_t = rope_tables()
    state = hidden
    for layer in range(2):
        a_act = rms_norm(state).astype(jnp.bfloat16)
        if layer == 0:
            k_proj = jnp.dot(a_act, w_key, preferred_element_type=jnp.float32).astype(jnp.bfloat16)
            k_cache = rope_norm(k_proj.reshape(SEQ, KV_HEADS, HEAD), cos_t, sin_t, k_gain)
            v_cache = jnp.dot(a_act, w_value, preferred_element_type=jnp.float32).astype(jnp.bfloat16).reshape(SEQ, KV_HEADS, HEAD)
        q_heads = jnp.dot(a_act, w_query[layer], preferred_element_type=jnp.float32).astype(jnp.bfloat16).reshape(SEQ, HEADS, HEAD)
        attn_out = attention(rope_norm(q_heads, cos_t, sin_t, q_gain[layer]), k_cache, v_cache)
        state = (state.astype(jnp.float32) + jnp.dot(attn_out, w_out[layer], preferred_element_type=jnp.float32)).astype(jnp.bfloat16)
        state = moe_block(state, routes[layer], w_router[layer], shared_gate[layer], shared_up[layer], shared_down[layer], expert_gate[layer], expert_up[layer], expert_down[layer])
    return (state, k_cache, v_cache)
```

```python
import functools
import math

import jax
import jax.numpy as jnp
from jax import lax
from jax.experimental import pallas as pl
from jax.experimental.pallas import tpu as pltpu
from jax.sharding import PartitionSpec as P

EPS = 1e-5
ROPE_BASE = 10000.0
TILE = 16
BLOCK_TILES = 16
GROUP = 4
SCORE_BOUND = 40.0
VALUE_BOUND = 1e15
NEG = -3e38
NT = (((1,), (1,)), ((), ()))
TN = (((0,), (0,)), ((), ()))


def rms_norm(vals):
    vals = vals.astype(jnp.float32)
    return vals * lax.rsqrt(jnp.mean(vals * vals, axis=-1, keepdims=True) + EPS)


def rope_tables_t(seq_len, head_dim):
    half_dim = head_dim // 2
    inv_freq = ROPE_BASE ** (-2.0 * jnp.arange(half_dim, dtype=jnp.float32) / head_dim)
    angles = inv_freq[:, None] * jnp.arange(seq_len, dtype=jnp.float32)[None, :]
    return jnp.cos(angles), jnp.sin(angles)


def rope_norm_t(raw, cos_t, sin_t, gain):
    vals = raw.astype(jnp.float32)
    half_dim = vals.shape[0] // 2
    first, second = vals[:half_dim], vals[half_dim:]
    rotated = jnp.concatenate([first * cos_t - second * sin_t, second * cos_t + first * sin_t], axis=0)
    scale = lax.rsqrt(jnp.mean(rotated * rotated, axis=0, keepdims=True) + EPS)
    return rotated * scale * gain


def qkv_kernel(a_ref, wq_ref, wk_ref, wv_ref, cos_ref, sin_ref, kg_ref, q_out, k_out, v_out, w_cat):
    nq, nk = wq_ref.shape[1], wk_ref.shape[0]

    @pl.when(pl.program_id(0) == 0)
    def _():
        w_cat[:nq, :] = wq_ref[0]
        w_cat[nq : nq + nk, :] = wk_ref[...]
        w_cat[nq + nk :, :] = wv_ref[...]

    res = lax.dot_general(w_cat[...], a_ref[...], NT, preferred_element_type=jnp.float32).astype(jnp.bfloat16)
    q_out[0] = res[:nq]
    k_out[...] = rope_norm_t(res[nq : nq + nk], cos_ref[...], sin_ref[...], kg_ref[...]).astype(jnp.bfloat16)
    v_out[...] = res[nq + nk :]


def qkv_proj(a_all, wq_t, wk_t, wv_t, cos_t, sin_t, k_gain, chunks):
    seq, dim = a_all.shape
    rows = seq // chunks
    nq, nk = wq_t.shape[1], wk_t.shape[0]
    half = cos_t.shape[0]
    return pl.pallas_call(
        qkv_kernel,
        grid=(chunks,),
        in_specs=[
            pl.BlockSpec((rows, dim), lambda i: (i, 0)),
            pl.BlockSpec((1, nq, dim), lambda i: (0, 0, 0)),
            pl.BlockSpec((nk, dim), lambda i: (0, 0)),
            pl.BlockSpec((nk, dim), lambda i: (0, 0)),
            pl.BlockSpec((half, rows), lambda i: (0, i)),
            pl.BlockSpec((half, rows), lambda i: (0, i)),
            pl.BlockSpec((nk, 1), lambda i: (0, 0)),
        ],
        out_specs=[
            pl.BlockSpec((1, nq, rows), lambda i: (i, 0, 0)),
            pl.BlockSpec((nk, rows), lambda i: (0, i)),
            pl.BlockSpec((nk, rows), lambda i: (0, i)),
        ],
        out_shape=[
            jax.ShapeDtypeStruct((chunks, nq, rows), jnp.bfloat16),
            jax.ShapeDtypeStruct((nk, seq), jnp.bfloat16),
            jax.ShapeDtypeStruct((nk, seq), jnp.bfloat16),
        ],
        scratch_shapes=[pltpu.VMEM((nq + 2 * nk, dim), jnp.bfloat16)],
        cost_estimate=pl.CostEstimate(flops=2 * seq * dim * (nq + 2 * nk), bytes_accessed=2 * seq * dim, transcendentals=0),
        name="qkv",
    )(a_all, wq_t, wk_t, wv_t, cos_t, sin_t, k_gain[:, None])


def attention_kernel(fast_ref, q_ref, k_ref, v_ref, cos_ref, sin_ref, qg_ref, out_ref, k2, q2, v_aug, acc, m_sc):
    step = pl.program_id(0)
    head_dim = k_ref.shape[0]
    rows = q_ref.shape[2]
    heads = q_ref.shape[1] // head_dim
    tile = rows // 2
    va = v_aug.shape[0]

    @pl.when(step == 0)
    def _():
        v_aug[...] = jnp.zeros_like(v_aug)

    here = pl.multiple_of(step * rows, rows)
    k_t = k_ref[:, pl.ds(here, rows)].astype(jnp.float32)
    k2[pl.ds(here, rows), :] = jnp.concatenate([k_t, k_t], axis=0).T.astype(jnp.bfloat16)
    v_aug[:head_dim, pl.ds(here, rows)] = v_ref[:, pl.ds(here, rows)]
    ones_row = lax.broadcasted_iota(jnp.int32, (va - head_dim, rows), 0) == 0
    v_aug[head_dim:, pl.ds(here, rows)] = jnp.where(ones_row, 1.0, 0.0).astype(jnp.bfloat16)

    for head in range(heads):
        raw = q_ref[0, head * head_dim : (head + 1) * head_dim, :]
        normed = rope_norm_t(raw, cos_ref[...], sin_ref[...], qg_ref[...]).astype(jnp.bfloat16)
        scaled = normed.astype(jnp.float32) * (head_dim**-0.5 * math.log2(math.e))
        high = scaled.astype(jnp.bfloat16)
        low = (scaled - high.astype(jnp.float32)).astype(jnp.bfloat16)
        q2[:head_dim, head * rows : (head + 1) * rows] = high
        q2[head_dim:, head * rows : (head + 1) * rows] = low

    acc[...] = jnp.zeros_like(acc)

    def columns(n):
        return slice(n * tile, (n + 1) * tile)

    def scores(start, n_keys, n):
        return jnp.dot(k2[pl.ds(start, n_keys), :], q2[:, columns(n)], preferred_element_type=jnp.float32)

    def masked(vals, half):
        key_pos = lax.broadcasted_iota(jnp.int32, vals.shape, 0)
        q_pos = lax.broadcasted_iota(jnp.int32, vals.shape, 1) + half * tile
        return jnp.where(key_pos <= q_pos, vals, NEG)

    def values(probs, start, n_keys):
        return jnp.dot(v_aug[:, pl.ds(start, n_keys)], probs.astype(jnp.bfloat16), preferred_element_type=jnp.float32)

    @pl.when(fast_ref[0] == 1)
    def _():
        def block(kb, carry):
            start = pl.multiple_of(kb * rows, rows)
            for n in range(2 * heads):
                acc[:, columns(n)] += values(jnp.exp2(scores(start, rows, n)), start, rows)
            return carry

        lax.fori_loop(0, step, block, 0)
        for n in range(2 * heads):
            n_keys = (n % 2 + 1) * tile
            acc[:, columns(n)] += values(jnp.exp2(masked(scores(here, n_keys, n), n % 2)), here, n_keys)

    @pl.when(fast_ref[0] != 1)
    def _():
        m_sc[...] = jnp.full_like(m_sc, NEG)

        def online(vals, start, n_keys, n):
            old = m_sc[0:1, columns(n)]
            new = jnp.maximum(old, jnp.max(vals, axis=0, keepdims=True))
            m_sc[0:1, columns(n)] = new
            acc[:, columns(n)] = acc[:, columns(n)] * jnp.exp2(old - new) + values(jnp.exp2(vals - new), start, n_keys)

        def block(kb, carry):
            start = pl.multiple_of(kb * rows, rows)
            for n in range(2 * heads):
                online(scores(start, rows, n), start, rows, n)
            return carry

        lax.fori_loop(0, step, block, 0)
        for n in range(2 * heads):
            n_keys = (n % 2 + 1) * tile
            online(masked(scores(here, n_keys, n), n % 2), here, n_keys, n)

    for head in range(heads):
        cols = slice(head * rows, (head + 1) * rows)
        out = acc[:head_dim, cols] / acc[head_dim : head_dim + 1, cols]
        out_ref[0, head * head_dim : (head + 1) * head_dim, :] = out.astype(jnp.bfloat16)


def attention(fast, q_raw, k_t, v_t, cos_t, sin_t, q_gain):
    chunks, nq, rows = q_raw.shape
    head_dim, seq = k_t.shape
    heads = nq // head_dim
    half = cos_t.shape[0]
    va = head_dim + 16
    pairs = heads * seq * seq // 2
    grid_spec = pltpu.PrefetchScalarGridSpec(
        num_scalar_prefetch=1,
        grid=(chunks,),
        in_specs=[
            pl.BlockSpec((1, nq, rows), lambda i, f: (i, 0, 0)),
            pl.BlockSpec((head_dim, seq), lambda i, f: (0, 0)),
            pl.BlockSpec((head_dim, seq), lambda i, f: (0, 0)),
            pl.BlockSpec((half, rows), lambda i, f: (0, i)),
            pl.BlockSpec((half, rows), lambda i, f: (0, i)),
            pl.BlockSpec((head_dim, 1), lambda i, f: (0, 0)),
        ],
        out_specs=pl.BlockSpec((1, nq, rows), lambda i, f: (i, 0, 0)),
        scratch_shapes=[
            pltpu.VMEM((seq, 2 * head_dim), jnp.bfloat16),
            pltpu.VMEM((2 * head_dim, heads * rows), jnp.bfloat16),
            pltpu.VMEM((va, seq), jnp.bfloat16),
            pltpu.VMEM((va, heads * rows), jnp.float32),
            pltpu.VMEM((8, heads * rows), jnp.float32),
        ],
    )
    return pl.pallas_call(
        attention_kernel,
        grid_spec=grid_spec,
        out_shape=jax.ShapeDtypeStruct((chunks, nq, rows), jnp.bfloat16),
        cost_estimate=pl.CostEstimate(flops=pairs * 256 * 4, bytes_accessed=8 * seq * nq, transcendentals=pairs),
        name="attention",
    )(fast, q_raw, k_t, v_t, cos_t, sin_t, q_gain[:, None])


def tile_lists(routes_all, chunks, n_experts):
    layers, seq = routes_all.shape
    rows = seq // chunks
    routes = routes_all.reshape(layers, chunks, rows)
    counts = jnp.sum((routes[..., None] == jnp.arange(n_experts)).astype(jnp.int32), axis=2)
    ends = jnp.cumsum(counts, axis=-1)
    offs = ends - counts
    first = offs // TILE
    n_tiles = jnp.where(counts > 0, (ends + TILE - 1) // TILE - first, 0)
    src = jnp.broadcast_to(jnp.arange(chunks)[None, :, None], counts.shape)

    def flat(vals):
        return jnp.swapaxes(vals, 1, 2).reshape(layers, 1, n_experts * chunks)

    n_tiles = flat(n_tiles)
    list_end = jnp.cumsum(n_tiles, axis=-1)
    list_off = list_end - n_tiles
    length = seq // TILE + chunks * n_experts + BLOCK_TILES
    pos = jnp.arange(length)[None, :, None]
    hit = (list_off <= pos) & (pos < list_end)

    def pick(vals):
        return jnp.sum(jnp.where(hit, vals, 0), axis=-1)

    entry = pick(pos - list_off + 1)
    valid = entry > 0
    local = pick(flat(first)) + entry - 1
    source = pick(flat(src))
    low = jnp.maximum(pick(flat(offs)) - local * TILE, 0)
    high = jnp.minimum(pick(flat(ends)) - local * TILE, TILE)
    tiles = jnp.where(valid, source * (rows // TILE) + local, 0)
    low = jnp.where(valid, low, 0)
    high = jnp.where(valid, high, 0)
    starts = list_off.reshape(layers, n_experts, chunks)[:, :, 0]
    stops = list_end.reshape(layers, n_experts, chunks)[:, :, -1]
    return tiles, low, high, starts, stops


def expert_kernel(tiles_ref, low_ref, high_ref, start_ref, stop_ref, n_hbm, p_hbm, sg_ref, su_ref, sd_ref, g_ref, u_ref, d_ref, out_hbm, n_all, p_all, out_all, w_in, w_out, lhs, fac, sems, out_sem):
    expert = pl.program_id(0)
    chunks = sems.shape[0] - 1
    rows = n_all.shape[0] // chunks
    width = g_ref.shape[2]
    n_rows = lhs.shape[0]
    dummy = n_all.shape[0]

    def n_copy(s):
        part = pl.ds(s * rows, rows)
        return pltpu.make_async_copy(n_hbm.at[pl.ds(s * (rows + TILE), rows), :], n_all.at[part, :], sems.at[s])

    p_copy = pltpu.make_async_copy(p_hbm, p_all, sems.at[chunks])

    @pl.when(expert == 0)
    def _():
        for s in range(chunks):
            n_copy(s).start()
        p_copy.start()
        w_in[width : 2 * width, :] = sg_ref[0]
        w_in[3 * width :, :] = su_ref[0]
        w_out[width : 2 * width, :] = sd_ref[0]
        w_out[3 * width :, :] = jnp.zeros_like(sd_ref[0])

        def clear(i, carry):
            out_all[pl.ds(pl.multiple_of(i * TILE, TILE), TILE), :] = jnp.zeros((TILE, out_all.shape[1]), out_all.dtype)
            return carry

        lax.fori_loop(0, out_all.shape[0] // TILE, clear, 0)
        for s in range(chunks):
            n_copy(s).wait()
        p_copy.wait()

    w_in[:width, :] = g_ref[0, 0]
    w_in[2 * width : 3 * width, :] = u_ref[0, 0]
    w_out[:width, :] = d_ref[0, 0]
    w_out[2 * width : 3 * width, :] = d_ref[0, 0]

    start, stop = start_ref[expert], stop_ref[expert]
    routed = lax.broadcasted_iota(jnp.int32, (TILE, 2 * width), 1) < width
    row_id = lax.broadcasted_iota(jnp.int32, (TILE, 2 * width), 0)

    def block(b, carry):
        first = start + b * BLOCK_TILES
        for j in range(BLOCK_TILES):
            idx = first + j
            at = pl.ds(pl.multiple_of(tiles_ref[idx] * TILE, TILE), TILE)
            mine = (row_id >= low_ref[idx]) & (row_id < jnp.where(idx < stop, high_ref[idx], 0))
            lhs[j * TILE : (j + 1) * TILE, :] = n_all[at, :]
            fac[j * TILE : (j + 1) * TILE, :] = jnp.where(mine, jnp.where(routed, p_all[at, :], 1.0), 0.0)
        both = lax.dot_general(lhs[...], w_in[...], NT, preferred_element_type=jnp.float32)
        gate, up = both[:, : 2 * width], both[:, 2 * width :]
        mid = (gate * jax.nn.sigmoid(gate) * up).astype(jnp.bfloat16).astype(jnp.float32) * fac[...]
        high = mid.astype(jnp.bfloat16)
        low = (mid - high.astype(jnp.float32)).astype(jnp.bfloat16)
        part = jnp.dot(jnp.concatenate([high, low], axis=1), w_out[...], preferred_element_type=jnp.float32).astype(jnp.bfloat16)
        for j0 in range(0, BLOCK_TILES, GROUP):
            places, sums = [], []
            for j in range(j0, j0 + GROUP):
                idx = first + j
                place = pl.ds(pl.multiple_of(jnp.where(idx < stop, tiles_ref[idx] * TILE, dummy), TILE), TILE)
                places.append(place)
                sums.append(out_all[place, :] + part[j * TILE : (j + 1) * TILE, :])
            for place, total in zip(places, sums):
                out_all[place, :] = total
        return carry

    lax.fori_loop(0, (stop - start + BLOCK_TILES - 1) // BLOCK_TILES, block, 0)

    @pl.when(expert == pl.num_programs(0) - 1)
    def _():
        copy = pltpu.make_async_copy(out_all.at[pl.ds(0, n_all.shape[0]), :], out_hbm, out_sem)
        copy.start()
        copy.wait()


def experts(lists, layer, n_all, p_all, s_gate, s_up, s_down, e_gate, e_up, e_down, chunks):
    _, n_experts, width, dim = e_gate.shape
    rows = n_all.shape[0] // chunks - TILE
    seq = rows * chunks
    n_rows = TILE * BLOCK_TILES
    shared = pl.BlockSpec((1, width, dim), lambda e, *_: (layer, 0, 0))
    routed = pl.BlockSpec((1, 1, width, dim), lambda e, *_: (layer, e, 0, 0))
    anywhere = pl.BlockSpec(memory_space=pl.ANY)
    grid_spec = pltpu.PrefetchScalarGridSpec(
        num_scalar_prefetch=5,
        grid=(n_experts,),
        in_specs=[anywhere, anywhere, shared, shared, shared, routed, routed, routed],
        out_specs=anywhere,
        scratch_shapes=[
            pltpu.VMEM((seq, dim), jnp.bfloat16),
            pltpu.VMEM((seq, 2 * width), jnp.float32),
            pltpu.VMEM((seq + TILE, dim), jnp.bfloat16),
            pltpu.VMEM((4 * width, dim), jnp.bfloat16),
            pltpu.VMEM((4 * width, dim), jnp.bfloat16),
            pltpu.VMEM((n_rows, dim), jnp.bfloat16),
            pltpu.VMEM((n_rows, 2 * width), jnp.float32),
            pltpu.SemaphoreType.DMA((chunks + 1,)),
            pltpu.SemaphoreType.DMA,
        ],
    )
    return pl.pallas_call(
        expert_kernel,
        grid_spec=grid_spec,
        out_shape=jax.ShapeDtypeStruct((seq, dim), jnp.bfloat16),
        compiler_params=pltpu.CompilerParams(vmem_limit_bytes=50 * 1024 * 1024),
        cost_estimate=pl.CostEstimate(flops=2 * 13500 * dim * 512, bytes_accessed=4 * seq * dim + 6 * n_experts * width * dim, transcendentals=0),
        name="experts",
    )(*lists, n_all, p_all, s_gate, s_up, s_down, e_gate, e_up, e_down)


def sort_rows(n_act, gate_val, route, n_experts):
    rows, dim = n_act.shape
    onehot = (route[:, None] == jnp.arange(n_experts)[None, :]).astype(jnp.bfloat16)
    earlier = (jnp.arange(rows)[:, None] > jnp.arange(rows)[None, :]).astype(jnp.bfloat16)
    rank = jnp.dot(earlier, onehot, preferred_element_type=jnp.float32)
    smaller = jnp.sum((route[None, :] < jnp.arange(n_experts)[:, None]).astype(jnp.float32), axis=1)
    pos = jnp.sum(onehot.astype(jnp.float32) * (rank + smaller[None, :]), axis=1).astype(jnp.int32)
    perm = pos[None, :] == jnp.arange(rows)[:, None]
    n_sorted = jnp.dot(perm.astype(jnp.bfloat16), n_act, preferred_element_type=jnp.float32).astype(jnp.bfloat16)
    gate_sorted = jnp.sum(jnp.where(perm, gate_val[None, :], 0.0), axis=1)
    high = gate_sorted.astype(jnp.bfloat16)
    low = (gate_sorted - high.astype(jnp.float32)).astype(jnp.bfloat16)
    extra = jnp.pad(jnp.concatenate([high, low])[None, :], ((0, TILE - 1), (0, dim - 2 * rows)))
    return jnp.concatenate([n_sorted, extra], axis=0), perm


def solution(mesh):
    seq_spec = P(("dp", "tp"), None)
    in_specs = (seq_spec, P(None, ("dp", "tp")), P(None, None, "tp"), P(None, "tp"), P(None, "tp"), P(None, "tp", None), P(None, None), P(None), P(None, None, None), P(None, None, "tp"), P(None, None, "tp"), P(None, "tp", None), P(None, None, None, "tp"), P(None, None, None, "tp"), P(None, None, "tp", None))
    out_specs = (seq_spec, P("dp", "tp", None), P("dp", "tp", None))
    chunks = mesh.shape["tp"]

    def per_device(hidden, routes, w_query, w_key, w_value, w_out, q_gain, k_gain, w_router, shared_gate, shared_up, shared_down, expert_gate, expert_up, expert_down):
        head_dim = q_gain.shape[1]
        n_experts = w_router.shape[2]
        rows, dim = hidden.shape
        seq_len = rows * chunks
        n_layers = w_query.shape[0]
        wq_t = jnp.swapaxes(w_query, 1, 2)
        s_gate, s_up = jnp.swapaxes(shared_gate, 1, 2), jnp.swapaxes(shared_up, 1, 2)
        e_gate, e_up = jnp.swapaxes(expert_gate, 2, 3), jnp.swapaxes(expert_up, 2, 3)

        routes_all = lax.all_gather(routes, "tp", axis=1, tiled=True)
        lists = tile_lists(routes_all, chunks, n_experts)
        cos_t, sin_t = rope_tables_t(seq_len, head_dim)

        a_all = lax.all_gather(rms_norm(hidden).astype(jnp.bfloat16), "tp", axis=0, tiled=True)
        q_raw, k_t, v_t = qkv_proj(a_all, wq_t, w_key.T, w_value.T, cos_t, sin_t, k_gain, chunks)
        small_v = jnp.max(jnp.abs(v_t)).astype(jnp.float32) <= VALUE_BOUND

        wq_t, w_out, q_raw = lax.optimization_barrier((wq_t, w_out, q_raw))
        wo_full = [lax.all_gather(w_out[layer], "tp", axis=0, tiled=True) for layer in range(n_layers)]
        wq_full = {layer: lax.all_gather(wq_t[layer], "tp", axis=0, tiled=True) for layer in range(1, n_layers)}

        state = hidden
        for layer in range(n_layers):
            if layer:
                a_act = rms_norm(state).astype(jnp.bfloat16)
                q_full = lax.dot_general(wq_full[layer], a_act, NT, preferred_element_type=jnp.float32).astype(jnp.bfloat16)
                q_raw = lax.all_to_all(q_full.reshape(chunks, -1, rows), "tp", 0, 0, tiled=True)
            bound = 1.02 * head_dim**0.5 * jnp.max(jnp.abs(q_gain[layer])) * jnp.max(jnp.abs(k_gain))
            fast = ((bound <= SCORE_BOUND) & small_v).astype(jnp.int32)[None]
            o_t = attention(fast, q_raw, k_t, v_t, cos_t, sin_t, q_gain[layer])
            o_t = lax.all_to_all(o_t, "tp", 0, 0, tiled=True).reshape(-1, rows)
            attn = lax.dot_general(o_t, wo_full[layer], TN, preferred_element_type=jnp.float32)
            state = (state.astype(jnp.float32) + attn).astype(jnp.bfloat16)

            n_act = rms_norm(state).astype(jnp.bfloat16)
            router_probs = jax.nn.softmax(jnp.dot(n_act, w_router[layer], preferred_element_type=jnp.float32), axis=-1)
            gate_val = jnp.sum(jnp.where(routes[layer][:, None] == jnp.arange(n_experts)[None, :], router_probs, 0.0), axis=1)
            payload, perm = sort_rows(n_act, gate_val, routes[layer], n_experts)
            n_all = lax.all_gather(payload, "tp", axis=0, tiled=True)
            gates = n_all.reshape(chunks, rows + TILE, dim)[:, rows, : 2 * rows].astype(jnp.float32)
            gates = (gates[:, :rows] + gates[:, rows:]).reshape(seq_len, 1)
            p_all = jnp.broadcast_to(gates, (seq_len, 2 * s_gate.shape[1]))
            part = experts([vals[layer] for vals in lists], layer, n_all, p_all, s_gate, s_up, shared_down, e_gate, e_up, expert_down, chunks)
            moe = lax.psum_scatter(part, "tp", scatter_dimension=0, tiled=True)
            moe = lax.dot_general(perm.astype(jnp.bfloat16), moe, TN, preferred_element_type=jnp.float32)
            state = (state.astype(jnp.float32) + moe).astype(jnp.bfloat16)
        return (state, k_t.T[:, None, :], v_t.T[:, None, :])

    return jax.shard_map(per_device, mesh=mesh, in_specs=in_specs, out_specs=out_specs, check_vma=False)
```
